32 devices in a mesh: tp: 8 (over z, y), dp: 4 (over x, core).
Axes of the slice: x: 2, y: 2, z: 4, core: 2. Of those that a mesh axis runs over, the one named last changes fastest.
Arguments:
- normed: bfloat16 [1024, 4096], P(('dp', 'tp')), may hold values from -6 to 6
- cotangent: bfloat16 [1024, 8192], P('dp', 'tp'), may hold values from -1.5 to 1.5
- weight_tiles: bfloat16 [2, 2048, 128, 128], P(None, 'tp'), may hold values from -0.09375 to 0.09375
- slot_tile: int32 [2048], replicated, may hold values from 0 to 2047, as said below
Outputs:
- hidden: bfloat16 [1024, 8192], P('dp', 'tp')
- d_normed: bfloat16 [1024, 4096], P(('dp', 'tp'))
- grad_tiles: float32 [2, 2048, 128, 128], P(None, 'tp', 'dp')
The draws below stay inside these ranges and needn't reach their ends.
Inputs may be any that keep to these rules, and one draw needn't show every extreme that they name: `slot_tile`: A permutation of 0 to 2047. Position p belongs to owner p // 256 at slot p % 256. Each owner holds 24 to 40 tiles of the tile columns t * 8 to (t + 1) * 8 - 1 of each index t of tp; in every draw some owner holds exactly 40 for some t.
All inputs are finite; a program needn't handle non-finite values.
Results may differ from the reference program's by a relative error of at most 0.018.
Values may be sent and summed in bfloat16 or wider, within the bound.
A program may use at most 128 MiB of HBM per device.

```python
import jax
import jax.numpy as jnp
from jax import lax

D = 4096
FW = 8192
TILE = 128
TOKENS = 1024
TR = 32
TC = 64
TPC = 8
NTILES = 2048
OWN = 256
N_DP = 4


def tile_layout(key):
    groups = TC // TPC
    owned_count = OWN
    base_count = owned_count // groups
    swing_count = base_count // 4
    key_offset, key_cons, key_owner = jax.random.split(jax.random.fold_in(key, 7), 3)
    offset_draw = jax.random.randint(key_offset, (), 0, groups)
    owner_axis = jnp.arange(groups)[:, None]
    cons_axis = jnp.arange(groups)[None, :]
    phase_step = (cons_axis - owner_axis + offset_draw) % groups
    counts = base_count + swing_count * (1 - 2 * (phase_step % 2))
    list_ends = jnp.cumsum(counts, axis=0)
    starts = list_ends - counts
    rank_ix = jnp.arange(owned_count)
    owner_of = jnp.sum((rank_ix[None, :, None] >= list_ends.T[:, None, :]).astype(jnp.int32), axis=2)
    index_in = rank_ix[None, :] - jnp.take_along_axis(starts.T, owner_of, axis=1)
    local_perm = jax.vmap(lambda sub: jax.random.permutation(sub, owned_count))(jax.random.split(key_cons, groups))
    cons_rows = jnp.broadcast_to(jnp.arange(groups)[:, None], (groups, owned_count))
    tile_row = local_perm // TPC
    tile_col = cons_rows * TPC + local_perm % TPC
    tile_id = (tile_row * TC + tile_col).astype(jnp.int32)
    offsets = jnp.cumsum(counts, axis=1) - counts
    pre_slot = offsets[owner_of, cons_rows] + index_in
    shuffles = jax.vmap(lambda sub: jax.random.permutation(sub, owned_count))(jax.random.split(key_owner, groups))
    slot_ix = shuffles[owner_of, pre_slot].astype(jnp.int32)
    slot_table = jnp.zeros((NTILES,), jnp.int32).at[(owner_of * owned_count + slot_ix).reshape(-1)].set(tile_id.reshape(-1))
    return slot_table


def draw_slot_tile(key, part):
    return tile_layout(key)


def shard_levels(stream_key, shape, cuts, low, high):
    factor_of, own = 1.0, jax.random.fold_in(stream_key, 6)
    for dim, shards_of in cuts:
        steps = jnp.exp(jax.random.uniform(jax.random.fold_in(own, dim), (shards_of,), jnp.float32, low / len(cuts), high / len(cuts)))
        factor_of = factor_of * jnp.repeat(steps, shape[dim] // shards_of).reshape([-1 if axis == dim else 1 for axis in range(len(shape))])
    return factor_of


def scatter_about(stream_key, shape, scale, reach, shards=(), kind=jnp.bfloat16):
    drawn = scale * jax.random.normal(stream_key, shape, jnp.float32)
    if shards:
        drawn = drawn * shard_levels(stream_key, shape, shards, -0.22, 0.18)
    return jnp.clip(drawn, -reach, reach).astype(kind)


def setup_inputs(seed: int = 0) -> dict:
    splits = jax.random.split(jax.random.key(seed), 5)
    normed = scatter_about(splits[0], (TOKENS, D), 1.0, 6.0, ((0, 32),))
    cotangent = scatter_about(splits[1], (TOKENS, FW), (8.0 / TOKENS ** 0.5), 1.5, ((0, 4), (1, 8)))
    weight_tiles = scatter_about(splits[2], (2, NTILES, TILE, TILE), D ** -0.5, 0.09375, ((1, 8),))
    slot_tile = draw_slot_tile(jax.random.fold_in(splits[4], 71), 0)
    return {"normed": normed, "cotangent": cotangent, "weight_tiles": weight_tiles, "slot_tile": slot_tile}


def reference(normed, cotangent, weight_tiles, slot_tile):
    by_number = jnp.zeros_like(weight_tiles).at[:, slot_tile].set(weight_tiles)
    weights = by_number.reshape(2, TR, TC, TILE, TILE).transpose(0, 1, 3, 2, 4).reshape(2, D, FW)
    gate_proj = jnp.dot(normed, weights[0], preferred_element_type=jnp.float32)
    up_proj = jnp.dot(normed, weights[1], preferred_element_type=jnp.float32)
    sigmoid_gate = jax.nn.sigmoid(gate_proj)
    act_gate = gate_proj * sigmoid_gate
    hidden = (act_gate * up_proj).astype(jnp.bfloat16)
    cot_full = cotangent.astype(jnp.float32)
    grad_gate = (cot_full * up_proj * (sigmoid_gate * (1.0 + gate_proj * (1.0 - sigmoid_gate)))).astype(jnp.bfloat16)
    grad_up = (cot_full * act_gate).astype(jnp.bfloat16)
    d_normed = (jnp.dot(grad_gate, weights[0].T, preferred_element_type=jnp.float32)
                + jnp.dot(grad_up, weights[1].T, preferred_element_type=jnp.float32)).astype(jnp.bfloat16)

    def replica(running, group_block):
        rows_in, rows_gate, rows_up = group_block
        part_gate = jnp.dot(rows_in.T, rows_gate, preferred_element_type=jnp.float32).astype(jnp.bfloat16)
        part_up = jnp.dot(rows_in.T, rows_up, preferred_element_type=jnp.float32).astype(jnp.bfloat16)
        stacked = lax.optimization_barrier(jnp.stack([part_gate, part_up]))
        return running + stacked.astype(jnp.float32), None

    start_sum = jnp.zeros((2, D, FW), jnp.float32)
    summed, _ = lax.scan(replica, start_sum, (normed.reshape(N_DP, -1, D), grad_gate.reshape(N_DP, -1, FW), grad_up.reshape(N_DP, -1, FW)))
    grad_tiled = summed.reshape(2, TR, TILE, TC, TILE).transpose(0, 1, 3, 2, 4).reshape(2, TR * TC, TILE, TILE)
    grad_tiles = grad_tiled[:, slot_tile]
    return hidden, d_normed, grad_tiles
```

```python
import jax
import jax.numpy as jnp
from jax import lax
from jax.experimental import pallas as pl
from jax.experimental.pallas import tpu as pltpu
from jax.sharding import PartitionSpec as P


def index_tables(slot_tile, groups, me, owned_count, tile_rows, tile_cols, list_len):
    cols_dev = tile_cols // groups
    tiles = slot_tile.reshape(groups, owned_count)
    target = tiles % tile_cols // cols_dev
    before = jnp.arange(owned_count)[:, None] < jnp.arange(owned_count)[None, :]
    ranks = jnp.arange(list_len, dtype=jnp.int32)
    devices = jnp.arange(groups, dtype=jnp.int32)
    my_target = lax.dynamic_index_in_dim(target, me, 0, keepdims=False)
    same = (my_target[:, None] == my_target[None, :]) & before
    my_rank = jnp.sum(same.astype(jnp.int32), axis=0)
    my_key = my_target * list_len + my_rank
    keys = (devices[:, None] * list_len + ranks[None, :]).reshape(-1)
    slots = jnp.arange(owned_count, dtype=jnp.int32)
    send_slots = jnp.sum(jnp.where(keys[:, None] == my_key[None, :], slots[None, :], 0), axis=1)
    mine = target == me
    rank = jnp.dot(
        mine.astype(jnp.bfloat16), before.astype(jnp.bfloat16), preferred_element_type=jnp.float32
    ).astype(jnp.int32)
    place = devices[:, None] * list_len + rank
    local_ix = (tiles % tile_cols - me * cols_dev) * tile_rows + tiles // tile_cols
    local_ix = jnp.where(mine, local_ix, -1)
    flat_local = local_ix.reshape(-1)
    blocks = jnp.arange(owned_count, dtype=jnp.int32)
    from_place = jnp.sum(
        jnp.where(blocks[:, None] == flat_local[None, :], place.reshape(-1)[None, :], 0), axis=1
    )
    hit = mine[:, None, :] & (rank[:, None, :] == ranks[None, :, None])
    return_ix = jnp.sum(jnp.where(hit, local_ix[:, None, :], 0), axis=2).reshape(-1)
    return send_slots, my_key, from_place, return_ix


def take_tiles(source, indices):
    flat = source.reshape((-1,) + source.shape[-2:])
    return jnp.take(flat, indices.reshape(-1), axis=0, mode="clip")


def project_kernel(banded_ref, weights_ref, out_ref):
    pair = jnp.concatenate([weights_ref[0], weights_ref[1]], axis=1)
    out_ref[...] = jnp.dot(
        banded_ref[...], pair, preferred_element_type=jnp.float32
    ).astype(out_ref.dtype)


def project(banded, weights):
    tokens, depth = banded.shape
    blocks, _, tile = weights.shape
    chunk = min(tokens, 1024)
    return pl.pallas_call(
        project_kernel,
        grid=(tokens // chunk, blocks // 2),
        in_specs=[
            pl.BlockSpec((chunk, depth), lambda n, b: (n, 0)),
            pl.BlockSpec((2, depth, tile), lambda n, b: (b, 0, 0)),
        ],
        out_specs=pl.BlockSpec((chunk, 2 * tile), lambda n, b: (n, b)),
        out_shape=jax.ShapeDtypeStruct((tokens, blocks * tile), jnp.bfloat16),
        cost_estimate=pl.CostEstimate(
            flops=2 * tokens * depth * blocks * tile,
            bytes_accessed=2 * (tokens * depth + depth * blocks * tile + tokens * blocks * tile),
            transcendentals=0,
        ),
    )(banded, weights)


def outer_kernel(banded_t_ref, grads_ref, out_ref, total_ref):
    step = pl.program_id(1)
    tile = out_ref.shape[2]
    term = jnp.dot(banded_t_ref[...], grads_ref[...], preferred_element_type=jnp.float32)

    @pl.when(step == 0)
    def _():
        total_ref[...] = term

    @pl.when(step > 0)
    def _():
        total_ref[...] += term

    @pl.when(step == pl.num_programs(1) - 1)
    def _():
        for half in range(2):
            part = total_ref[:, half * tile : (half + 1) * tile]
            out_ref[half] = part.astype(out_ref.dtype)


def outer(banded_t, grads, tile):
    depth, tokens = banded_t.shape
    blocks = grads.shape[1] // tile
    chunk = min(tokens, 1024)
    return pl.pallas_call(
        outer_kernel,
        grid=(blocks // 2, tokens // chunk),
        in_specs=[
            pl.BlockSpec((depth, chunk), lambda b, n: (0, n)),
            pl.BlockSpec((chunk, 2 * tile), lambda b, n: (n, b)),
        ],
        out_specs=pl.BlockSpec((2, depth, tile), lambda b, n: (b, 0, 0)),
        out_shape=jax.ShapeDtypeStruct((blocks, depth, tile), jnp.bfloat16),
        scratch_shapes=[pltpu.VMEM((depth, 2 * tile), jnp.float32)],
        cost_estimate=pl.CostEstimate(
            flops=2 * tokens * depth * blocks * tile,
            bytes_accessed=2 * (tokens * depth + depth * blocks * tile + tokens * blocks * tile),
            transcendentals=0,
        ),
    )(banded_t, grads)


def local(normed, cotangent, weight_tiles, slot_tile):
    tp_size = lax.axis_size("tp")
    dp_size = lax.axis_size("dp")
    me_tp = lax.axis_index("tp")
    me_dp = lax.axis_index("dp")
    rows, width = normed.shape
    group_rows, cols = cotangent.shape
    owned_count, tile = weight_tiles.shape[1:3]
    tile_rows = width // tile
    cols_dev = cols // tile
    tile_cols = cols_dev * tp_size
    base_count = owned_count // tp_size
    list_len = base_count + base_count // 4
    band = tile // dp_size
    depth = tile_rows * band
    tokens = group_rows * dp_size
    send_slots, my_key, from_place, return_ix = index_tables(
        slot_tile, tp_size, me_tp, owned_count, tile_rows, tile_cols, list_len
    )

    by_band = normed.reshape(rows, tile_rows, dp_size, band).transpose(2, 0, 1, 3)
    by_band = by_band.reshape(dp_size, rows, depth)
    by_group = lax.all_to_all(by_band, "dp", split_axis=0, concat_axis=0, tiled=True)
    banded = lax.all_gather(by_group, "tp", axis=1, tiled=True).reshape(tokens, depth)

    both = jnp.arange(2, dtype=jnp.int32)
    send_ix = send_slots.reshape(tp_size, 1, list_len) + both[None, :, None] * owned_count
    in_ix = (from_place // list_len * 2 + both[:, None]) * list_len + from_place % list_len
    back_ix = return_ix.reshape(tp_size, 1, list_len) + both[None, :, None] * owned_count
    out_ix = (my_key // list_len * 2 + both[:, None]) * list_len + my_key % list_len
    travel = (tp_size, 2 * list_len, band, tile)
    own_rows = lax.dynamic_slice_in_dim(weight_tiles, me_dp * band, band, 2)
    outgoing = take_tiles(own_rows, send_ix).reshape(travel)
    arrived = lax.all_to_all(outgoing, "tp", split_axis=0, concat_axis=0, tiled=True)
    weights = take_tiles(arrived, in_ix).reshape(2 * cols_dev, depth, tile)

    partial = project(banded, weights)
    proj = lax.psum_scatter(partial, "dp", scatter_dimension=0, tiled=True).astype(jnp.float32)
    gate_proj = proj[:, :cols]
    up_proj = proj[:, cols:]
    sigmoid_gate = jax.nn.sigmoid(gate_proj)
    act_gate = gate_proj * sigmoid_gate
    hidden = (act_gate * up_proj).astype(jnp.bfloat16)
    cot_full = cotangent.astype(jnp.float32)
    grad_gate = (
        cot_full * up_proj * (sigmoid_gate * (1.0 + gate_proj * (1.0 - sigmoid_gate)))
    ).astype(jnp.bfloat16)
    grad_up = (cot_full * act_gate).astype(jnp.bfloat16)
    grads = jnp.concatenate([grad_gate, grad_up], axis=1)
    grads = lax.all_gather(grads, "dp", axis=0, tiled=True)

    summed = outer(banded.T, grads, tile).reshape(2 * owned_count, band, tile)
    back = take_tiles(summed, back_ix).reshape(travel)
    back, grads = lax.optimization_barrier((back, grads))
    returned = lax.all_to_all(back, "tp", split_axis=0, concat_axis=0, tiled=True)
    result = take_tiles(returned, out_ix).astype(jnp.float32)
    result = result.reshape(2, owned_count, band, tile)

    grads = grads.reshape(tokens, 2 * cols_dev, tile)
    term = jnp.einsum("nbj,bkj->nk", grads, weights, preferred_element_type=jnp.float32)
    term = term.astype(jnp.bfloat16).reshape(dp_size, tp_size, rows, depth).transpose(1, 0, 2, 3)
    d_band = lax.psum_scatter(term.reshape(-1, depth), "tp", scatter_dimension=0, tiled=True)
    d_band = d_band.reshape(dp_size, rows, depth)
    d_rows = lax.all_to_all(d_band, "dp", split_axis=0, concat_axis=0, tiled=True)
    d_normed = d_rows.reshape(dp_size, rows, tile_rows, band).transpose(1, 2, 0, 3)
    return (hidden, d_normed.reshape(rows, width), result)


def solution(mesh):
    return jax.shard_map(
        local,
        mesh=mesh,
        in_specs=(P(("dp", "tp"), None), P("dp", "tp"), P(None, "tp", None, None), P()),
        out_specs=(P("dp", "tp"), P(("dp", "tp"), None), P(None, "tp", "dp", None)),
        check_vma=False,
    )
```

```python
import jax
import jax.numpy as jnp
from jax import lax
from jax.experimental import pallas as pl
from jax.experimental.pallas import tpu as pltpu
from jax.sharding import PartitionSpec as P


def index_tables(slot_tile, groups, me, owned_count, tile_rows, tile_cols, list_len):
    cols_dev = tile_cols // groups
    tiles = slot_tile.reshape(groups, owned_count)
    target = tiles % tile_cols // cols_dev
    before = jnp.arange(owned_count)[:, None] < jnp.arange(owned_count)[None, :]
    ranks = jnp.arange(list_len, dtype=jnp.int32)
    devices = jnp.arange(groups, dtype=jnp.int32)
    my_target = lax.dynamic_index_in_dim(target, me, 0, keepdims=False)
    same = (my_target[:, None] == my_target[None, :]) & before
    my_rank = jnp.sum(same.astype(jnp.int32), axis=0)
    my_key = my_target * list_len + my_rank
    keys = (devices[:, None] * list_len + ranks[None, :]).reshape(-1)
    slots = jnp.arange(owned_count, dtype=jnp.int32)
    send_slots = jnp.sum(jnp.where(keys[:, None] == my_key[None, :], slots[None, :], 0), axis=1)
    mine = target == me
    rank = jnp.dot(
        mine.astype(jnp.bfloat16), before.astype(jnp.bfloat16), preferred_element_type=jnp.float32
    ).astype(jnp.int32)
    place = devices[:, None] * list_len + rank
    local_ix = (tiles % tile_cols - me * cols_dev) * tile_rows + tiles // tile_cols
    local_ix = jnp.where(mine, local_ix, -1)
    flat_local = local_ix.reshape(-1)
    blocks = jnp.arange(owned_count, dtype=jnp.int32)
    from_place = jnp.sum(
        jnp.where(blocks[:, None] == flat_local[None, :], place.reshape(-1)[None, :], 0), axis=1
    )
    hit = mine[:, None, :] & (rank[:, None, :] == ranks[None, :, None])
    return_ix = jnp.sum(jnp.where(hit, local_ix[:, None, :], 0), axis=2).reshape(-1)
    return send_slots, my_key, from_place, return_ix


def take_tiles(source, indices):
    flat = source.reshape((-1,) + source.shape[-2:])
    return jnp.take(flat, indices.reshape(-1), axis=0, mode="clip")


def project_kernel(banded_ref, weights_ref, out_ref):
    pair = jnp.concatenate([weights_ref[0], weights_ref[1]], axis=1)
    out_ref[...] = jnp.dot(
        banded_ref[...], pair, preferred_element_type=jnp.float32
    ).astype(out_ref.dtype)


def project(banded, weights):
    tokens, depth = banded.shape
    blocks, _, tile = weights.shape
    chunk = min(tokens, 1024)
    return pl.pallas_call(
        project_kernel,
        grid=(tokens // chunk, blocks // 2),
        in_specs=[
            pl.BlockSpec((chunk, depth), lambda n, b: (n, 0)),
            pl.BlockSpec((2, depth, tile), lambda n, b: (b, 0, 0)),
        ],
        out_specs=pl.BlockSpec((chunk, 2 * tile), lambda n, b: (n, b)),
        out_shape=jax.ShapeDtypeStruct((tokens, blocks * tile), jnp.bfloat16),
        cost_estimate=pl.CostEstimate(
            flops=2 * tokens * depth * blocks * tile,
            bytes_accessed=2 * (tokens * depth + depth * blocks * tile + tokens * blocks * tile),
            transcendentals=0,
        ),
    )(banded, weights)


def outer_kernel(banded_t_ref, grads_ref, out_ref, total_ref):
    step = pl.program_id(1)
    tile = out_ref.shape[2]
    term = jnp.dot(banded_t_ref[...], grads_ref[...], preferred_element_type=jnp.float32)

    @pl.when(step == 0)
    def _():
        total_ref[...] = term

    @pl.when(step > 0)
    def _():
        total_ref[...] += term

    @pl.when(step == pl.num_programs(1) - 1)
    def _():
        for half in range(2):
            part = total_ref[:, half * tile : (half + 1) * tile]
            out_ref[half] = part.astype(out_ref.dtype)


def outer(banded_t, grads, tile):
    depth, tokens = banded_t.shape
    blocks = grads.shape[1] // tile
    chunk = min(tokens, 1024)
    return pl.pallas_call(
        outer_kernel,
        grid=(blocks // 2, tokens // chunk),
        in_specs=[
            pl.BlockSpec((depth, chunk), lambda b, n: (0, n)),
            pl.BlockSpec((chunk, 2 * tile), lambda b, n: (n, b)),
        ],
        out_specs=pl.BlockSpec((2, depth, tile), lambda b, n: (b, 0, 0)),
        out_shape=jax.ShapeDtypeStruct((blocks, depth, tile), jnp.bfloat16),
        scratch_shapes=[pltpu.VMEM((depth, 2 * tile), jnp.float32)],
        cost_estimate=pl.CostEstimate(
            flops=2 * tokens * depth * blocks * tile,
            bytes_accessed=2 * (tokens * depth + depth * blocks * tile + tokens * blocks * tile),
            transcendentals=0,
        ),
    )(banded_t, grads)


def local(normed, cotangent, weight_tiles, slot_tile):
    tp_size = lax.axis_size("tp")
    dp_size = lax.axis_size("dp")
    me_tp = lax.axis_index("tp")
    me_dp = lax.axis_index("dp")
    rows, width = normed.shape
    group_rows, cols = cotangent.shape
    owned_count, tile = weight_tiles.shape[1:3]
    tile_rows = width // tile
    cols_dev = cols // tile
    tile_cols = cols_dev * tp_size
    base_count = owned_count // tp_size
    list_len = base_count + base_count // 4
    band = tile // dp_size
    depth = tile_rows * band
    tokens = group_rows * dp_size
    send_slots, my_key, from_place, return_ix = index_tables(
        slot_tile, tp_size, me_tp, owned_count, tile_rows, tile_cols, list_len
    )

    by_band = normed.reshape(rows, tile_rows, dp_size, band).transpose(2, 0, 1, 3)
    by_band = by_band.reshape(dp_size, rows, depth)
    by_group = lax.all_to_all(by_band, "dp", split_axis=0, concat_axis=0, tiled=True)
    banded = lax.all_gather(by_group, "tp", axis=1, tiled=True).reshape(tokens, depth)

    travel = (tp_size, list_len, band, tile)
    own_rows = [
        lax.dynamic_slice(
            weight_tiles, (m, 0, me_dp * band, 0), (1, owned_count, band, tile)
        )
        for m in range(2)
    ]
    outgoing = [take_tiles(own_rows[m], send_slots).reshape(travel) for m in range(2)]
    weights, proj = [], []
    for m in range(2):
        with jax.named_scope(f"send{m}"):
            arrived = lax.all_to_all(outgoing[m], "tp", split_axis=0, concat_axis=0, tiled=True)
        with jax.named_scope(f"proj{m}"):
            weights.append(take_tiles(arrived, from_place).reshape(cols_dev, depth, tile))
            partial = project(banded, weights[m])
            proj.append(
                lax.psum_scatter(partial, "dp", scatter_dimension=0, tiled=True).astype(jnp.float32)
            )
    gate_proj, up_proj = proj
    sigmoid_gate = jax.nn.sigmoid(gate_proj)
    act_gate = gate_proj * sigmoid_gate
    hidden = (act_gate * up_proj).astype(jnp.bfloat16)
    cot_full = cotangent.astype(jnp.float32)
    grad_gate = (
        cot_full * up_proj * (sigmoid_gate * (1.0 + gate_proj * (1.0 - sigmoid_gate)))
    ).astype(jnp.bfloat16)
    grad_up = (cot_full * act_gate).astype(jnp.bfloat16)
    grads = [lax.all_gather(g, "dp", axis=0, tiled=True) for g in (grad_gate, grad_up)]
    banded_t = banded.T
    back = []
    for m in range(2):
        with jax.named_scope(f"outer{m}"):
            summed = outer(banded_t, grads[m], tile).reshape(owned_count, band, tile)
            back.append(take_tiles(summed, return_ix).reshape(travel))
    back[1], grads[0], grads[1] = lax.optimization_barrier((back[1], grads[0], grads[1]))
    result = []
    for m in range(2):
        with jax.named_scope(f"back{m}"):
            returned = lax.all_to_all(back[m], "tp", split_axis=0, concat_axis=0, tiled=True)
        result.append(take_tiles(returned, my_key).reshape(owned_count, band, tile))
    result = jnp.stack(result).astype(jnp.float32)

    with jax.named_scope("term"):
        term = sum(
            jnp.einsum(
                "nbj,bkj->nk",
                grads[m].reshape(tokens, cols_dev, tile),
                weights[m],
                preferred_element_type=jnp.float32,
            )
            for m in range(2)
        )
        term = term.astype(jnp.bfloat16).reshape(dp_size, tp_size, rows, depth)
        term = term.transpose(1, 0, 2, 3)
    d_band = lax.psum_scatter(term.reshape(-1, depth), "tp", scatter_dimension=0, tiled=True)
    d_band = d_band.reshape(dp_size, rows, depth)
    d_all = lax.all_gather(d_band, "dp", axis=0, tiled=False)
    d_rows = lax.dynamic_index_in_dim(d_all, me_dp, 1, keepdims=False)
    d_normed = d_rows.reshape(dp_size, rows, tile_rows, band).transpose(1, 2, 0, 3)
    return (hidden, d_normed.reshape(rows, width), result)


def solution(mesh):
    return jax.shard_map(
        local,
        mesh=mesh,
        in_specs=(P(("dp", "tp"), None), P("dp", "tp"), P(None, "tp", None, None), P()),
        out_specs=(P("dp", "tp"), P(("dp", "tp"), None), P(None, "tp", "dp", None)),
        check_vma=False,
    )
```
